256 devices in a mesh: atoms: 64 (over z_hi, y, x, core), gsplit: 4 (over z_lo).
Axes of the slice: x: 4, y: 4, z: 8 (z_hi: 2, z_lo: 4; z = z_hi * 4 + z_lo), core: 2. Of those that a mesh axis runs over, the one named last changes fastest.
Arguments:
- miller: int32 [3, 30720], P(None, 'gsplit'), may hold values from -16 to 16, as said below
- form_factors: bfloat16 [49, 30720], P(None, 'gsplit'), may hold values from -6 to 6
- fractional: float32 [3, 4096], P(None, 'atoms'), may hold values from 0 to 1
- multipoles: bfloat16 [2, 49, 4096], P(None, None, 'atoms'), may hold values from -0.013671875 to 0.013671875
- point_owner: int32 [8192], P(('atoms', 'gsplit')), may hold values from 0 to 63
- offsets: float32 [3, 8192], P(None, ('atoms', 'gsplit')), may hold values from -0.05 to 0.05
Outputs:
- grid_potential: float32 [2, 8192], P(None, ('atoms', 'gsplit'))
- moments: float32 [2, 49, 4096], P(None, None, ('atoms', 'gsplit'))
The draws below stay inside these ranges and needn't reach their ends.
Inputs may be any that keep to these rules, and one draw needn't show every extreme that they name: `miller`: no vector has all three indices zero. Point p belongs to atom (p // 128) * 64 + point_owner[p].
All inputs are finite; a program needn't handle non-finite values.
Results may differ from the reference program's by a relative error of at most 0.0045.
Values may be sent and summed in bfloat16 or wider, within the bound.
No kernel may reach another device: no remote copies, remote signals or barrier semaphores. Data moves between devices by JAX's collectives and lax.ppermute only.
A program may use at most 64 MiB of HBM per device.

```python
import math
import jax
import jax.numpy as jnp
from jax import lax

COMPS = 49
NG = 30720
DENS = 2
ATOM_BLK = 64
ATOMS = 4096
P_BLK = 128
POINTS = 8192


def draw_miller(key, part):
    values = jax.random.randint(jax.random.fold_in(key, 11), (3, NG), -16, 17, dtype=jnp.int32)
    all_zero = jnp.all(values == 0, axis=0)
    first_row = jnp.where(all_zero, 1, values[0]).astype(jnp.int32)
    return jnp.concatenate([first_row[None, :], values[1:]], axis=0).astype(jnp.int32)


def set_ends(values, key, least, high):
    longest = values.shape.index(max(values.shape))
    spots = []
    for shift in (0, 1):
        where = [jax.random.randint(jax.random.fold_in(key, axis), (), 0, length) for axis, length in enumerate(values.shape)]
        where[longest] = (where[longest] + shift) % values.shape[longest]
        spots.append(tuple(where))
    return values.at[spots[0]].set(least).at[spots[1]].set(high)


def shard_levels(rng, dims, cuts, smallest, high):
    factor_of, own = 1.0, jax.random.fold_in(rng, 6)
    for dim, parts in cuts:
        steps = jnp.exp(jax.random.uniform(jax.random.fold_in(own, dim), (parts,), jnp.float32, smallest / len(cuts), high / len(cuts)))
        factor_of = factor_of * jnp.repeat(steps, dims[dim] // parts).reshape([-1 if axis == dim else 1 for axis in range(len(dims))])
    return factor_of


def normal_values(key, dims, scale, bound, split=(), kind=jnp.bfloat16):
    drawn = jax.random.normal(key, dims, jnp.float32) * scale
    if len(split) > 0:
        drawn = shard_levels(key, dims, split, -0.22, 0.18) * drawn
    return jnp.clip(drawn, min=-bound, max=bound).astype(kind)


def setup_inputs(seed: int = 0) -> dict:
    keys = jax.random.split(jax.random.key(seed), 7)
    miller = draw_miller(jax.random.fold_in(keys[6], 71), 0)
    form_factors = normal_values(keys[1], (COMPS, NG), 1.0, 6.0, ((1, 4),))
    fractional = jnp.clip(1.0 * jax.random.uniform(keys[2], (3, ATOMS), jnp.float32) ** shard_levels(keys[2], (3, ATOMS), ((1, 64),), -0.2, 0.2), 0.0, 1.0)
    multipoles = normal_values(keys[3], (DENS, COMPS, ATOMS), (ATOMS * COMPS) ** -0.5, 0.013671875, ((2, 64),))
    point_owner = set_ends(jax.random.randint(keys[4], (POINTS,), 0, ATOM_BLK), jax.random.fold_in(keys[4], 1), 0, ATOM_BLK - 1).astype(jnp.int32)
    offsets = jnp.clip(jax.random.uniform(keys[5], (3, POINTS), jnp.float32, -0.05, 0.05) * shard_levels(keys[5], (3, POINTS), ((1, 256),), -0.4, 0.0), -0.05, 0.05)
    return dict(miller=miller, form_factors=form_factors, fractional=fractional, multipoles=multipoles, point_owner=point_owner, offsets=offsets)


two_pi = 2.0 * math.pi
damping = 1.0 / 400.0


def angles(vectors, places):
    indices = vectors.astype(jnp.float32)
    summed = places[0][:, None] * indices[0][None, :] + places[1][:, None] * indices[1][None, :] + places[2][:, None] * indices[2][None, :]
    return two_pi * summed


def sign_tables(comp_count):
    comp_ids = jnp.arange(comp_count, dtype=jnp.int32)
    degree = jnp.zeros((comp_count,), jnp.int32)
    for degree_step in range(1, 16):
        degree = degree + (comp_ids >= degree_step * degree_step).astype(jnp.int32)
    quarter = degree % 4
    even_sign = jnp.where(quarter == 0, 1.0, jnp.where(quarter == 2, -1.0, 0.0)).astype(jnp.float32)
    odd_sign = jnp.where(quarter == 3, 1.0, jnp.where(quarter == 1, -1.0, 0.0)).astype(jnp.float32)
    return even_sign, odd_sign


def coulomb(vectors):
    indices = vectors.astype(jnp.float32)
    square = indices[0] * indices[0] + indices[1] * indices[1] + indices[2] * indices[2]
    return jnp.exp(-damping * square) / square


def structure(multipoles, cos_table, sin_table, form_block, even_sign, odd_sign):
    density_count, comp_count, atom_count = multipoles.shape
    flattened = multipoles.reshape(density_count * comp_count, atom_count)
    along_cos = jnp.dot(flattened, cos_table, preferred_element_type=jnp.float32).reshape(density_count, comp_count, -1)
    along_sin = jnp.dot(flattened, sin_table, preferred_element_type=jnp.float32).reshape(density_count, comp_count, -1)
    weights = form_block.astype(jnp.float32)[None]
    even_wide = even_sign[None, :, None]
    odd_wide = odd_sign[None, :, None]
    real_part = jnp.sum(weights * (even_wide * along_cos + odd_wide * along_sin), axis=1)
    imag_part = jnp.sum(weights * (odd_wide * along_cos - even_wide * along_sin), axis=1)
    return jnp.stack([real_part, imag_part], axis=1)


def moment_terms(potential, form_block, cos_table, sin_table, even_sign, odd_sign):
    weighted = (form_block.astype(jnp.float32)[None, None] * potential[:, :, None, :]).astype(jnp.bfloat16)
    density_count, _, comp_count, vector_count = weighted.shape
    flattened = weighted.reshape(density_count * 2 * comp_count, vector_count)
    contract = (((1,), (1,)), ((), ()))
    with_cos = lax.dot_general(flattened, cos_table, contract, preferred_element_type=jnp.float32).reshape(density_count, 2, comp_count, -1)
    with_sin = lax.dot_general(flattened, sin_table, contract, preferred_element_type=jnp.float32).reshape(density_count, 2, comp_count, -1)
    even_wide = even_sign[None, :, None]
    odd_wide = odd_sign[None, :, None]
    return even_wide * with_cos[:, 0] + odd_wide * with_sin[:, 0] + odd_wide * with_cos[:, 1] - even_wide * with_sin[:, 1]


def grid_rows(rounded, vectors, places):
    point_angles = angles(vectors, places)
    cos_points = jnp.cos(point_angles).astype(jnp.bfloat16)
    sin_points = jnp.sin(point_angles).astype(jnp.bfloat16)
    contract = (((1,), (1,)), ((), ()))
    return lax.dot_general(cos_points, rounded[:, 0], contract, preferred_element_type=jnp.float32) - lax.dot_general(sin_points, rounded[:, 1], contract, preferred_element_type=jnp.float32)


def reference(miller, form_factors, fractional, multipoles, point_owner, offsets):
    even_sign, odd_sign = sign_tables(COMPS)
    blocks = 32
    block_width = NG // blocks
    point_index = jnp.arange(POINTS, dtype=jnp.int32)
    owner_index = ((point_index // P_BLK) * ATOM_BLK + point_owner).astype(jnp.int32)
    places = jnp.take(fractional, owner_index, axis=1) + offsets
    vector_blocks = miller.reshape(3, blocks, block_width).transpose(1, 0, 2)
    form_blocks = form_factors.reshape(COMPS, blocks, block_width).transpose(1, 0, 2)

    def advance(carried, pieces):
        moment_sum, grid_sum = carried
        vectors, form_block = pieces
        phases = angles(vectors, fractional)
        cos_table = jnp.cos(phases).astype(jnp.bfloat16)
        sin_table = jnp.sin(phases).astype(jnp.bfloat16)
        summed = structure(multipoles, cos_table, sin_table, form_block, even_sign, odd_sign)
        potential = coulomb(vectors)[None, None, :] * summed
        moment_sum = moment_sum + moment_terms(potential, form_block, cos_table, sin_table, even_sign, odd_sign)
        grid_sum = grid_sum + grid_rows(potential.astype(jnp.bfloat16), vectors, places)
        return (moment_sum, grid_sum), None

    initial = (jnp.zeros((DENS, COMPS, ATOMS), jnp.float32), jnp.zeros((POINTS, DENS), jnp.float32))
    (moment_sum, grid_sum), _ = lax.scan(advance, initial, (vector_blocks, form_blocks))
    return grid_sum.T, moment_sum
```

```python
import functools
import itertools

import jax
import jax.numpy as jnp
import numpy as np
from jax import lax
from jax.experimental import pallas as pl
from jax.experimental.pallas import tpu as pltpu
from jax.sharding import Mesh
from jax.sharding import PartitionSpec as P


damping = 1.0 / 400.0
AXES = ("zh", "y", "x", "c", "g")
SIZES = {"zh": 2, "y": 4, "x": 4, "c": 2, "g": 4}
ROWS = 56

SIN = (4.442883014678955, -7.308245658874512, 3.606353998184204, -0.8461104035377502, 0.10982204228639603)
COS = (1.4142135381698608, -6.978850841522217, 5.73945951461792, -1.8835527896881104, 0.3106778562068939)


def exchanged(value, **flips):
    axes = tuple(axis for axis in AXES if axis in flips)
    sizes = [SIZES[axis] for axis in axes]
    pairs = []
    for place in itertools.product(*[range(size) for size in sizes]):
        other = [at ^ flips[axis] for at, axis in zip(place, axes)]
        flat = lambda spot: functools.reduce(lambda done, pair: done * pair[1] + pair[0], zip(spot, sizes), 0)
        pairs.append((flat(place), flat(other)))
    return lax.ppermute(value, axes, pairs)


def turns(columns, indices):
    angle = columns[0] * indices[0] + columns[1] * indices[1] + columns[2] * indices[2]
    rest = angle - jnp.round(angle)
    square = rest * rest
    sine = SIN[4]
    cosine = COS[4]
    for power in (3, 2, 1, 0):
        sine = sine * square + SIN[power]
        cosine = cosine * square + COS[power]
    sine = sine * rest
    return 1.0 - sine * sine, sine * cosine


def degree_signs(comp_count):
    degree = np.floor(np.sqrt(np.arange(comp_count))).astype(np.int64)
    quarter = degree % 4
    even = np.where(quarter == 0, 1.0, np.where(quarter == 2, -1.0, 0.0)).astype(np.float32)
    odd = np.where(quarter == 3, 1.0, np.where(quarter == 1, -1.0, 0.0)).astype(np.float32)
    return even, odd


def column(ref, axis):
    return ref[:, axis : axis + 1]


def half_start(flip, width):
    half = lax.axis_index("c")
    if flip:
        half = 1 - half
    return half * width


def tables_into(table_ref, columns, miller_ref, base, start, count):
    vectors = miller_ref[:, pl.ds(pl.multiple_of(base + start, 128), 128)].astype(jnp.float32)
    indices = [vectors[axis : axis + 1, :] for axis in range(3)]
    for low in range(0, count, 64):
        part = [values[low : low + 64] for values in columns]
        cosine, sine = turns(part, indices)
        spot = pl.ds(pl.multiple_of(start, 128), 128)
        table_ref[low : low + 64, spot] = cosine.astype(jnp.bfloat16)
        table_ref[count + low : count + low + 64, spot] = sine.astype(jnp.bfloat16)


def structure_kernel(flip, miller_ref, form_ref, frac_ref, lhs_ref, table_ref, sums_ref):
    width = table_ref.shape[1]
    comps = form_ref.shape[0]
    base = half_start(flip, width)
    columns = [column(frac_ref, axis) for axis in range(3)]
    atoms = frac_ref.shape[0]
    unroll = 5

    def step(index, carry):
        for inner in range(unroll):
            start = (index * unroll + inner) * 256
            for part in range(2):
                tables_into(table_ref, columns, miller_ref, base, start + 128 * part, atoms)
            spot = pl.ds(pl.multiple_of(start, 256), 256)
            along = jnp.dot(lhs_ref[...], table_ref[:, spot], preferred_element_type=jnp.float32)
            form = form_ref[:, pl.ds(pl.multiple_of(base + start, 128), 256)].astype(jnp.float32)
            for row in range(4):
                part = along[ROWS * row : ROWS * row + comps]
                sums_ref[row : row + 1, spot] = jnp.sum(form * part, axis=0, keepdims=True)
        return carry

    lax.fori_loop(0, width // (256 * unroll), step, 0)


def points_kernel(flip, miller_ref, places_ref, table_ref):
    width = table_ref.shape[1]
    base = half_start(flip, width)
    turned = places_ref[...].T
    columns = [turned[:, axis : axis + 1] for axis in range(3)]
    count = turned.shape[0]
    unroll = 5

    def step(index, carry):
        for inner in range(unroll):
            tables_into(table_ref, columns, miller_ref, base, (index * unroll + inner) * 128, count)
        return carry

    lax.fori_loop(0, width // (128 * unroll), step, 0)


def moments_kernel(flip, comps, *refs):
    if flip:
        miller_ref, form_ref, sums_ref, atoms_ref, points_ref, before_ref, out_ref, form_scr, cos_scr, sin_scr = refs
    else:
        miller_ref, form_ref, sums_ref, atoms_ref, points_ref, out_ref, form_scr, cos_scr, sin_scr = refs
    width = atoms_ref.shape[1]
    base = half_start(flip, width)
    rows = lax.broadcasted_iota(jnp.int32, (ROWS, 128), 0)
    even = rows == comps
    for degree in range(0, 16, 2):
        even = even | ((rows >= degree * degree) & (rows < min((degree + 1) * (degree + 1), comps)))
    ones = (lax.broadcasted_iota(jnp.int32, (ROWS - comps, 128), 0) == 0).astype(jnp.float32)
    unroll = 5

    def step(index, carry):
        for inner in range(unroll):
            start = (index * unroll + inner) * 128
            spot = pl.ds(pl.multiple_of(start, 128), 128)
            there = pl.ds(pl.multiple_of(base + start, 128), 128)
            vectors = miller_ref[:, there].astype(jnp.float32)
            square = jnp.sum(vectors * vectors, axis=0, keepdims=True)
            kernel = jnp.exp(-damping * square) / square
            potential = kernel * sums_ref[:, spot]
            form_scr[inner, 0:comps, :] = form_ref[:, there].astype(jnp.float32)
            form_scr[inner, comps:ROWS, :] = ones
            form = form_scr[inner]
            against_cos, against_sin = [], []
            for density in range(2):
                real = potential[2 * density : 2 * density + 1]
                imag = potential[2 * density + 1 : 2 * density + 2]
                against_cos.append(form * jnp.where(even, real, imag))
                against_sin.append(form * jnp.where(even, -imag, real))
            cos_scr[:, spot] = jnp.concatenate(against_cos, axis=0).astype(jnp.bfloat16)
            sin_scr[:, spot] = jnp.concatenate(against_sin, axis=0).astype(jnp.bfloat16)
        return carry

    lax.fori_loop(0, width // (128 * unroll), step, 0)
    atoms = atoms_ref.shape[0] // 2
    points = points_ref.shape[0] // 2
    contract = (((1,), (1,)), ((), ()))
    total = None
    for part, weights in enumerate((cos_scr, sin_scr)):
        table = jnp.concatenate(
            [atoms_ref[atoms * part : atoms * (part + 1)], points_ref[points * part : points * (part + 1)]], axis=0
        )
        term = lax.dot_general(weights[...], table, contract, preferred_element_type=jnp.float32)
        total = term if total is None else total + term
    if flip:
        total = total + before_ref[...]
    out_ref[...] = total


def cost(flops):
    return pl.CostEstimate(flops=flops, bytes_accessed=1 << 20, transcendentals=0)


PARAMS = pltpu.CompilerParams(vmem_limit_bytes=24 << 20)


def relative(value, axis, own):
    lengths = value.shape
    quarters = value.reshape(*lengths[:axis], 2, 2, lengths[axis] // 4, *lengths[axis + 1 :])
    quarters = jnp.where((own // 2) == 0, quarters, jnp.flip(quarters, axis))
    quarters = jnp.where((own % 2) == 0, quarters, jnp.flip(quarters, axis + 1))
    return quarters.reshape(lengths)


def shards(miller, form_factors, fractional, multipoles, point_owner, offsets):
    comps, vectors = form_factors.shape
    atoms = fractional.shape[1]
    half = vectors // 2
    own = lax.axis_index("g")
    even, odd = degree_signs(comps)

    atom_ids = jnp.arange(atoms, dtype=jnp.int32)
    onehot = (atom_ids[:, None] == point_owner[None, :]).astype(jnp.float32)
    places = jnp.dot(fractional, onehot, precision=lax.Precision.HIGHEST, preferred_element_type=jnp.float32) + offsets
    places = jnp.concatenate([places, jnp.zeros((5, places.shape[1]), jnp.float32)], axis=0)
    places = jnp.concatenate([places, exchanged(places, g=1)], axis=1)
    places = jnp.concatenate([places, exchanged(places, g=2)], axis=1)

    frac = relative(fractional, 1, own).T
    moved = relative(multipoles, 2, own)
    by_cos = np.stack([even, odd])[None, :, :, None].astype(jnp.bfloat16)
    by_sin = np.stack([odd, -even])[None, :, :, None].astype(jnp.bfloat16)
    lhs = jnp.concatenate([moved[:, None] * by_cos, moved[:, None] * by_sin], axis=3)
    lhs = jnp.pad(lhs, ((0, 0), (0, 0), (0, ROWS - comps), (0, 0))).reshape(4 * ROWS, 2 * atoms)

    def structure(flip):
        return pl.pallas_call(
            functools.partial(structure_kernel, flip),
            out_shape=(
                jax.ShapeDtypeStruct((2 * atoms, half), jnp.bfloat16),
                jax.ShapeDtypeStruct((4, half), jnp.float32),
            ),
            compiler_params=PARAMS,
            cost_estimate=cost(2 * half * 128 * 224 * 8),
            name="structure%d" % flip,
        )(miller, form_factors, frac, lhs)

    def point_table(flip):
        return pl.pallas_call(
            functools.partial(points_kernel, flip),
            out_shape=jax.ShapeDtypeStruct((2 * places.shape[1], half), jnp.bfloat16),
            compiler_params=PARAMS,
            cost_estimate=cost(2 * half * 128 * 224 * 8),
            name="points%d" % flip,
        )(miller, places)

    far_table, far_sums = structure(1)
    arrived = exchanged(far_sums, c=1)
    near_table, near_sums = structure(0)
    sums = near_sums + arrived
    far_points = point_table(1)
    near_points = point_table(0)
    for stage in (
        [dict(zh=1)],
        [dict(y=1, x=1), dict(x=1), dict(y=1)],
        [dict(y=3, x=3), dict(x=3), dict(y=3)],
    ):
        parts = [exchanged(sums, **flips) for flips in stage]
        for part in parts:
            sums = sums + part
    other_sums = exchanged(sums, c=1)

    def contract(flip, summed, atom_table, points, before):
        return pl.pallas_call(
            functools.partial(moments_kernel, flip, comps),
            out_shape=jax.ShapeDtypeStruct((2 * ROWS, atoms + places.shape[1]), jnp.float32),
            scratch_shapes=[
                pltpu.VMEM((5, ROWS, 128), jnp.float32),
                pltpu.VMEM((2 * ROWS, half), jnp.bfloat16),
                pltpu.VMEM((2 * ROWS, half), jnp.bfloat16),
            ],
            compiler_params=PARAMS,
            cost_estimate=cost(2 * half * 256 * 112 * 8),
            name="moments%d" % flip,
        )(miller, form_factors, summed, atom_table, points, *before)

    near = contract(0, sums, near_table, near_points, ())
    total = contract(1, other_sums, far_table, far_points, (near,))

    own_atoms = atoms // 4
    own_points = places.shape[1] // 4
    piece = lambda turn: jnp.concatenate(
        [
            total[:, own_atoms * turn : own_atoms * (turn + 1)],
            total[:, atoms + own_points * turn : atoms + own_points * (turn + 1)],
        ],
        axis=1,
    )
    summed = piece(0)
    for part in [exchanged(piece(turn), g=turn) for turn in (3, 2, 1)]:
        summed = summed + part
    summed = summed.reshape(2, ROWS, own_atoms + own_points)
    moments = summed[:, :comps, :own_atoms] * (even + odd)[None, :, None]
    return summed[:, comps, own_atoms:], moments


def solution(mesh):
    fine = Mesh(mesh.devices.reshape([SIZES[axis] for axis in AXES]), AXES)
    block = ("zh", "y", "x", "c")
    placed = (
        P(None, "g"),
        P(None, "g"),
        P(None, block),
        P(None, None, block),
        P(AXES),
        P(None, AXES),
    )
    return jax.shard_map(
        shards,
        mesh=fine,
        in_specs=placed,
        out_specs=(P(None, AXES), P(None, None, AXES)),
        check_vma=False,
    )
```

```python
import functools
import itertools

import jax
import jax.numpy as jnp
from jax import lax
from jax.experimental import pallas as pl
from jax.experimental.pallas import tpu as pltpu
from jax.sharding import Mesh
from jax.sharding import PartitionSpec as P


damping = 1.0 / 400.0
AXES = ("zh", "y", "x", "c", "g")
SIZES = {"zh": 2, "y": 4, "x": 4, "c": 2, "g": 4}
ROWS = 56

SIN = (4.442883014678955, -7.308245658874512, 3.606353998184204, -0.8461104035377502, 0.10982204228639603)
COS = (1.4142135381698608, -6.978850841522217, 5.73945951461792, -1.8835527896881104, 0.3106778562068939)


def exchanged(value, **flips):
    axes = tuple(axis for axis in AXES if axis in flips)
    sizes = [SIZES[axis] for axis in axes]
    pairs = []
    for place in itertools.product(*[range(size) for size in sizes]):
        other = [at ^ flips[axis] for at, axis in zip(place, axes)]
        flat = lambda spot: functools.reduce(lambda done, pair: done * pair[1] + pair[0], zip(spot, sizes), 0)
        pairs.append((flat(place), flat(other)))
    return lax.ppermute(value, axes, pairs)


def turns(columns, indices):
    angle = columns[0] * indices[0] + columns[1] * indices[1] + columns[2] * indices[2]
    rest = angle - jnp.round(angle)
    square = rest * rest
    sine = SIN[4]
    cosine = COS[4]
    for power in (3, 2, 1, 0):
        sine = sine * square + SIN[power]
        cosine = cosine * square + COS[power]
    sine = sine * rest
    return 1.0 - sine * sine, sine * cosine


def half_start(flip, width):
    half = lax.axis_index("c")
    if flip:
        half = 1 - half
    return half * width


def tables_into(table_ref, columns, miller_ref, base, start, count):
    vectors = miller_ref[:, pl.ds(pl.multiple_of(base + start, 128), 128)].astype(jnp.float32)
    indices = [vectors[axis : axis + 1, :] for axis in range(3)]
    for low in range(0, count, 64):
        part = [values[low : low + 64] for values in columns]
        cosine, sine = turns(part, indices)
        spot = pl.ds(pl.multiple_of(start, 128), 128)
        table_ref[low : low + 64, spot] = cosine.astype(jnp.bfloat16)
        table_ref[count + low : count + low + 64, spot] = sine.astype(jnp.bfloat16)


def row_signs(comps, lanes):
    rows = lax.broadcasted_iota(jnp.int32, (comps, lanes), 0)
    even = jnp.zeros((comps, lanes), jnp.float32)
    odd = jnp.zeros((comps, lanes), jnp.float32)
    degree = 0
    while degree * degree < comps:
        here = (rows >= degree * degree) & (rows < (degree + 1) * (degree + 1))
        sign = (1.0, -1.0, -1.0, 1.0)[degree % 4]
        if degree % 2 == 0:
            even = jnp.where(here, sign, even)
        else:
            odd = jnp.where(here, sign, odd)
        degree += 1
    return even, odd


def structure_into(base, columns, lhs, miller_ref, form_ref, table_ref, sums_ref, form_ready):
    width = table_ref.shape[1]
    comps = form_ref.shape[0]
    for start in range(0, width, 256):
        cosines, sines = [], []
        for part in range(2):
            there = pl.ds(pl.multiple_of(base + start + 128 * part, 128), 128)
            vectors = miller_ref[:, there].astype(jnp.float32)
            cosine, sine = turns(columns, [vectors[axis : axis + 1, :] for axis in range(3)])
            cosines.append(cosine.astype(jnp.bfloat16))
            sines.append(sine.astype(jnp.bfloat16))
        table = jnp.concatenate([jnp.concatenate(cosines, axis=1), jnp.concatenate(sines, axis=1)], axis=0)
        table_ref[:, start : start + 256] = table
        along = jnp.dot(lhs, table, preferred_element_type=jnp.float32)
        if start == 0:
            form_ready()
        form = form_ref[:, pl.ds(pl.multiple_of(base + start, 128), 256)].astype(jnp.float32)
        for row in range(4):
            part = along[ROWS * row : ROWS * row + comps]
            sums_ref[row : row + 1, start : start + 256] = jnp.sum(form * part, axis=0, keepdims=True)


def first_kernel(
    miller_hbm, form_hbm, frac_hbm, poles_hbm, owner_hbm, offsets_hbm,
    table_ref, sums_ref, places_ref, miller_ref, form_ref, lhs_ref, frac_ref,
    frac_in, poles_ref, owner_ref, offsets_ref, lhs_scr, sems,
):
    width = table_ref.shape[1]
    comps = form_ref.shape[0]
    atoms = frac_in.shape[1]
    base = half_start(True, width)
    other = half_start(False, width)
    far = pl.ds(pl.multiple_of(base, 128), width)
    near = pl.ds(pl.multiple_of(other, 128), width)
    moves = [
        (frac_hbm, frac_in),
        (poles_hbm, poles_ref),
        (miller_hbm, miller_ref),
        (form_hbm.at[:, far], form_ref.at[:, far]),
        (owner_hbm, owner_ref),
        (offsets_hbm, offsets_ref),
        (form_hbm.at[:, near], form_ref.at[:, near]),
    ]
    copies = [pltpu.make_async_copy(start, end, sems.at[spot]) for spot, (start, end) in enumerate(moves)]
    for copy in copies:
        copy.start()
    frac_ref[...] = jnp.zeros_like(frac_ref)
    lhs_scr[...] = jnp.zeros_like(lhs_scr)
    places_ref[...] = jnp.zeros_like(places_ref)
    even, odd = row_signs(comps, atoms)
    copies[0].wait()
    frac_ref[0:3, 0:atoms] = frac_in[...]
    turned = frac_ref[...].T
    columns = [turned[0:atoms, axis : axis + 1] for axis in range(3)]
    copies[1].wait()
    for density in range(2):
        poles = poles_ref[:, density, :].astype(jnp.float32)
        low = 2 * ROWS * density
        lhs_scr[low : low + comps, :] = jnp.concatenate([poles * even, poles * odd], axis=1)
        lhs_scr[low + ROWS : low + ROWS + comps, :] = jnp.concatenate([poles * odd, -(poles * even)], axis=1)
    lhs = lhs_scr[...].astype(jnp.bfloat16)
    lhs_ref[...] = lhs
    copies[2].wait()
    structure_into(base, columns, lhs, miller_ref, form_ref, table_ref, sums_ref, copies[3].wait)
    copies[4].wait()
    copies[5].wait()
    points = owner_ref.shape[1]
    chosen = lax.broadcasted_iota(jnp.int32, (atoms, points), 0) == owner_ref[...]
    for axis in range(3):
        spread = jnp.where(chosen, columns[axis], 0.0)
        places_ref[axis : axis + 1, :] = jnp.sum(spread, axis=0, keepdims=True) + offsets_ref[axis : axis + 1, :]
    copies[6].wait()


def second_kernel(miller_ref, form_ref, lhs_ref, frac_ref, table_ref, sums_ref):
    atoms = table_ref.shape[0] // 2
    base = half_start(False, table_ref.shape[1])
    turned = frac_ref[...].T
    columns = [turned[0:atoms, axis : axis + 1] for axis in range(3)]
    structure_into(base, columns, lhs_ref[...], miller_ref, form_ref, table_ref, sums_ref, lambda: None)


def points_kernel(flip, miller_ref, places_ref, table_ref):
    width = table_ref.shape[1]
    base = half_start(flip, width)
    turned = places_ref[...].T
    columns = [turned[:, axis : axis + 1] for axis in range(3)]
    count = turned.shape[0]
    unroll = 5

    def step(index, carry):
        for inner in range(unroll):
            tables_into(table_ref, columns, miller_ref, base, (index * unroll + inner) * 128, count)
        return carry

    lax.fori_loop(0, width // (128 * unroll), step, 0)


def moments_kernel(flip, comps, *refs):
    miller_ref, form_ref, sums_ref, atoms_ref, points_ref = refs[:5]
    if flip:
        before_ref, refs = refs[5], refs[6:]
        outs, (form_scr, cos_scr, sin_scr, turned_scr) = refs[:4], refs[4:]
    else:
        out_ref, form_scr, cos_scr, sin_scr = refs[5:]
    width = atoms_ref.shape[1]
    base = half_start(flip, width)
    rows = lax.broadcasted_iota(jnp.int32, (ROWS, 128), 0)
    even = rows == comps
    for degree in range(0, 16, 2):
        even = even | ((rows >= degree * degree) & (rows < min((degree + 1) * (degree + 1), comps)))
    ones = (lax.broadcasted_iota(jnp.int32, (ROWS - comps, 128), 0) == 0).astype(jnp.float32)
    atoms = atoms_ref.shape[0] // 2
    points = points_ref.shape[0] // 2
    contract = (((1,), (1,)), ((), ()))
    total = before_ref[...] if flip else None
    chunk = width // 3
    for slot in range(form_scr.shape[0]):
        form_scr[slot, comps:ROWS, :] = ones
    for first in range(0, width, chunk):
        for start in range(first, first + chunk, 128):
            there = pl.ds(pl.multiple_of(base + start, 128), 128)
            vectors = miller_ref[:, there].astype(jnp.float32)
            square = jnp.sum(vectors * vectors, axis=0, keepdims=True)
            kernel = jnp.exp(-damping * square) / square
            potential = kernel * sums_ref[:, start : start + 128]
            slot = (start // 128) % form_scr.shape[0]
            form_scr[slot, 0:comps, :] = form_ref[:, there].astype(jnp.float32)
            form = form_scr[slot]
            against_cos, against_sin = [], []
            for density in range(2):
                real = potential[2 * density : 2 * density + 1]
                imag = potential[2 * density + 1 : 2 * density + 2]
                against_cos.append(form * jnp.where(even, real, imag))
                against_sin.append(form * jnp.where(even, -imag, real))
            cos_scr[:, start : start + 128] = jnp.concatenate(against_cos, axis=0).astype(jnp.bfloat16)
            sin_scr[:, start : start + 128] = jnp.concatenate(against_sin, axis=0).astype(jnp.bfloat16)
        span = slice(first, first + chunk)
        for part, weights in enumerate((cos_scr, sin_scr)):
            table = jnp.concatenate(
                [
                    atoms_ref[atoms * part : atoms * (part + 1), span],
                    points_ref[points * part : points * (part + 1), span],
                ],
                axis=0,
            )
            term = lax.dot_general(weights[:, span], table, contract, preferred_element_type=jnp.float32)
            total = term if total is None else total + term
    if not flip:
        out_ref[...] = total
        return
    pad = jnp.zeros((2 * ROWS, turned_scr.shape[0] - atoms - points), jnp.float32)
    turned_scr[...] = jnp.concatenate([total, pad], axis=1).T
    own = lax.axis_index("g")
    for turn, out_ref in enumerate(outs):
        few = atoms // 4
        many = points // 4
        out_ref[0:few] = turned_scr[pl.ds(pl.multiple_of((own ^ turn) * few, few), few)]
        out_ref[few : few + many] = turned_scr[atoms + many * turn : atoms + many * (turn + 1)]


def finish_kernel(comps, atoms, first_ref, second_ref, third_ref, fourth_ref, grid_ref, moments_ref):
    total = (first_ref[...] + second_ref[...]) + (third_ref[...] + fourth_ref[...])
    turned = total.T
    place = lax.broadcasted_iota(jnp.int32, (atoms, comps), 1)
    sign = jnp.zeros((atoms, comps), jnp.float32)
    degree = 0
    while degree * degree < comps:
        here = (place >= degree * degree) & (place < (degree + 1) * (degree + 1))
        sign = jnp.where(here, (1.0, -1.0, -1.0, 1.0)[degree % 4], sign)
        degree += 1
    for density in range(2):
        low = ROWS * density
        moments_ref[density] = total[0:atoms, low : low + comps] * sign
        grid_ref[density : density + 1, :] = turned[low + comps : low + comps + 1, atoms:]


def cost(flops):
    return pl.CostEstimate(flops=flops, bytes_accessed=1 << 20, transcendentals=0)


PARAMS = pltpu.CompilerParams(vmem_limit_bytes=24 << 20)


def shards(miller, form_factors, fractional, multipoles, point_owner, offsets):
    comps, vectors = form_factors.shape
    atoms = fractional.shape[1]
    half = vectors // 2
    own_points = offsets.shape[1]
    points = 4 * own_points
    few = atoms // 4
    shape = jax.ShapeDtypeStruct

    table_shapes = (shape((2 * atoms, half), jnp.bfloat16), shape((4, half), jnp.float32))
    structure_cost = cost(2 * half * 128 * 224 * 8)
    far_table, far_sums, places, miller, form_factors, lhs, frac = pl.pallas_call(
        first_kernel,
        in_specs=[pl.BlockSpec(memory_space=pltpu.HBM)] * 6,
        out_shape=(
            *table_shapes,
            shape((8, own_points), jnp.float32),
            shape(miller.shape, miller.dtype),
            shape(form_factors.shape, form_factors.dtype),
            shape((4 * ROWS, 2 * atoms), jnp.bfloat16),
            shape((8, 128), jnp.float32),
        ),
        scratch_shapes=[
            pltpu.VMEM((3, atoms), jnp.float32),
            pltpu.VMEM((comps, 2, atoms), jnp.bfloat16),
            pltpu.VMEM((1, own_points), jnp.int32),
            pltpu.VMEM((3, own_points), jnp.float32),
            pltpu.VMEM((4 * ROWS, 2 * atoms), jnp.float32),
            pltpu.SemaphoreType.DMA((7,)),
        ],
        compiler_params=PARAMS,
        cost_estimate=structure_cost,
        name="structure1",
    )(
        *[
            pltpu.with_memory_space_constraint(value, pltpu.HBM)
            for value in (
                miller, form_factors, fractional, jnp.transpose(multipoles, (1, 0, 2)), point_owner[None], offsets
            )
        ]
    )

    arrived = exchanged(far_sums, c=1)
    places = jnp.concatenate([places, exchanged(places, g=1)], axis=1)
    near_table, near_sums = pl.pallas_call(
        second_kernel,
        out_shape=table_shapes,
        compiler_params=PARAMS,
        cost_estimate=structure_cost,
        name="structure0",
    )(miller, form_factors, lhs, frac)
    sums = near_sums + arrived
    sums, places = lax.optimization_barrier((sums, places))

    def point_table(flip):
        return pl.pallas_call(
            functools.partial(points_kernel, flip),
            out_shape=shape((2 * points, half), jnp.bfloat16),
            compiler_params=PARAMS,
            cost_estimate=cost(2 * half * 128 * 224 * 8),
        )(miller, places)

    crossed = exchanged(sums, zh=1)
    others = exchanged(places, g=2)
    places = jnp.concatenate([places, others], axis=1)
    sums = sums + crossed
    far_points = point_table(1)
    near_points = point_table(0)
    for stage in (
        [dict(y=1, x=1), dict(x=1), dict(y=1)],
        [dict(y=3, x=3), dict(x=3), dict(y=3)],
    ):
        parts = [exchanged(sums, **flips) for flips in stage]
        for part in parts:
            sums = sums + part
    other_sums = exchanged(sums, c=1)

    def contract(flip, summed, atom_table, point_rows, before):
        if flip:
            out_shape = [shape((few + own_points, 2 * ROWS), jnp.float32)] * 4
            more = [pltpu.VMEM((256, 2 * ROWS), jnp.float32)]
        else:
            out_shape = shape((2 * ROWS, atoms + points), jnp.float32)
            more = []
        return pl.pallas_call(
            functools.partial(moments_kernel, flip, comps),
            out_shape=out_shape,
            scratch_shapes=[
                pltpu.VMEM((5, ROWS, 128), jnp.float32),
                pltpu.VMEM((2 * ROWS, half), jnp.bfloat16),
                pltpu.VMEM((2 * ROWS, half), jnp.bfloat16),
                *more,
            ],
            compiler_params=PARAMS,
            cost_estimate=cost(2 * half * 256 * 112 * 8),
        )(miller, form_factors, summed, atom_table, point_rows, *before)

    near = contract(0, sums, near_table, near_points, ())
    pieces = contract(1, other_sums, far_table, far_points, (near,))
    pieces = [pieces[0]] + [exchanged(pieces[turn], g=turn) for turn in (1, 2, 3)]
    grid, moments = pl.pallas_call(
        functools.partial(finish_kernel, comps, few),
        out_shape=[shape((2, own_points), jnp.float32), shape((2, few, comps), jnp.float32)],
        compiler_params=PARAMS,
        cost_estimate=cost(1 << 20),
        name="finish",
    )(*pieces)
    return grid, jnp.transpose(moments, (0, 2, 1))


def solution(mesh):
    fine = Mesh(mesh.devices.reshape([SIZES[axis] for axis in AXES]), AXES)
    block = ("zh", "y", "x", "c")
    placed = (
        P(None, "g"),
        P(None, "g"),
        P(None, block),
        P(None, None, block),
        P(AXES),
        P(None, AXES),
    )
    return jax.shard_map(
        shards,
        mesh=fine,
        in_specs=placed,
        out_specs=(P(None, AXES), P(None, None, AXES)),
        check_vma=False,
    )
```

```python
import functools
import itertools

import jax
import jax.numpy as jnp
from jax import lax
from jax.experimental import pallas as pl
from jax.experimental.pallas import tpu as pltpu
from jax.sharding import Mesh
from jax.sharding import PartitionSpec as P


damping = 1.0 / 400.0
AXES = ("zh", "y", "x", "c", "g")
SIZES = {"zh": 2, "y": 4, "x": 4, "c": 2, "g": 4}
ROWS = 56

SIN = (4.442883014678955, -7.308245658874512, 3.606353998184204, -0.8461104035377502, 0.10982204228639603)
COS = (1.4142135381698608, -6.978850841522217, 5.73945951461792, -1.8835527896881104, 0.3106778562068939)


def exchanged(value, **flips):
    axes = tuple(axis for axis in AXES if axis in flips)
    sizes = [SIZES[axis] for axis in axes]
    pairs = []
    for place in itertools.product(*[range(size) for size in sizes]):
        other = [at ^ flips[axis] for at, axis in zip(place, axes)]
        flat = lambda spot: functools.reduce(lambda done, pair: done * pair[1] + pair[0], zip(spot, sizes), 0)
        pairs.append((flat(place), flat(other)))
    return lax.ppermute(value, axes, pairs)


def turns(columns, indices):
    angle = columns[0] * indices[0] + columns[1] * indices[1] + columns[2] * indices[2]
    rest = angle - jnp.round(angle)
    square = rest * rest
    sine = SIN[4]
    cosine = COS[4]
    for power in (3, 2, 1, 0):
        sine = sine * square + SIN[power]
        cosine = cosine * square + COS[power]
    sine = sine * rest
    return 1.0 - sine * sine, sine * cosine


def half_start(flip, width):
    half = lax.axis_index("c")
    if flip:
        half = 1 - half
    return half * width


def tables_into(table_ref, columns, miller_ref, base, start, count):
    vectors = miller_ref[:, pl.ds(pl.multiple_of(base + start, 128), 128)].astype(jnp.float32)
    indices = [vectors[axis : axis + 1, :] for axis in range(3)]
    for low in range(0, count, 64):
        part = [values[low : low + 64] for values in columns]
        cosine, sine = turns(part, indices)
        spot = pl.ds(pl.multiple_of(start, 128), 128)
        table_ref[low : low + 64, spot] = cosine.astype(jnp.bfloat16)
        table_ref[count + low : count + low + 64, spot] = sine.astype(jnp.bfloat16)


def row_signs(comps, lanes):
    rows = lax.broadcasted_iota(jnp.int32, (comps, lanes), 0)
    even = jnp.zeros((comps, lanes), jnp.float32)
    odd = jnp.zeros((comps, lanes), jnp.float32)
    degree = 0
    while degree * degree < comps:
        here = (rows >= degree * degree) & (rows < (degree + 1) * (degree + 1))
        sign = (1.0, -1.0, -1.0, 1.0)[degree % 4]
        if degree % 2 == 0:
            even = jnp.where(here, sign, even)
        else:
            odd = jnp.where(here, sign, odd)
        degree += 1
    return even, odd


def structure_into(base, columns, lhs, miller_ref, form_ref, table_ref, sums_ref, form_ready):
    width = table_ref.shape[1]
    comps = form_ref.shape[0]
    for start in range(0, width, 256):
        cosines, sines = [], []
        for part in range(2):
            there = pl.ds(pl.multiple_of(base + start + 128 * part, 128), 128)
            vectors = miller_ref[:, there].astype(jnp.float32)
            cosine, sine = turns(columns, [vectors[axis : axis + 1, :] for axis in range(3)])
            cosines.append(cosine.astype(jnp.bfloat16))
            sines.append(sine.astype(jnp.bfloat16))
        table = jnp.concatenate([jnp.concatenate(cosines, axis=1), jnp.concatenate(sines, axis=1)], axis=0)
        table_ref[:, start : start + 256] = table
        along = jnp.dot(lhs, table, preferred_element_type=jnp.float32)
        if start == 0:
            form_ready()
        form = form_ref[:, pl.ds(pl.multiple_of(base + start, 128), 256)].astype(jnp.float32)
        for row in range(4):
            part = along[ROWS * row : ROWS * row + comps]
            sums_ref[row : row + 1, start : start + 256] = jnp.sum(form * part, axis=0, keepdims=True)


def first_kernel(
    miller_hbm, form_hbm, frac_hbm, poles_hbm, owner_hbm, offsets_hbm,
    table_ref, sums_ref, places_ref, miller_ref, form_ref, lhs_ref, frac_ref,
    frac_in, poles_ref, owner_ref, offsets_ref, lhs_scr, sems,
):
    width = table_ref.shape[1]
    comps = form_ref.shape[0]
    atoms = frac_in.shape[1]
    base = half_start(True, width)
    other = half_start(False, width)
    far = pl.ds(pl.multiple_of(base, 128), width)
    near = pl.ds(pl.multiple_of(other, 128), width)
    moves = [
        (frac_hbm, frac_in),
        (poles_hbm, poles_ref),
        (miller_hbm, miller_ref),
        (form_hbm.at[:, far], form_ref.at[:, far]),
        (owner_hbm, owner_ref),
        (offsets_hbm, offsets_ref),
        (form_hbm.at[:, near], form_ref.at[:, near]),
    ]
    copies = [pltpu.make_async_copy(start, end, sems.at[spot]) for spot, (start, end) in enumerate(moves)]
    for copy in copies:
        copy.start()
    frac_ref[...] = jnp.zeros_like(frac_ref)
    lhs_scr[...] = jnp.zeros_like(lhs_scr)
    places_ref[...] = jnp.zeros_like(places_ref)
    even, odd = row_signs(comps, atoms)
    copies[0].wait()
    frac_ref[0:3, 0:atoms] = frac_in[...]
    turned = frac_ref[...].T
    columns = [turned[0:atoms, axis : axis + 1] for axis in range(3)]
    copies[1].wait()
    for density in range(2):
        poles = poles_ref[:, density, :].astype(jnp.float32)
        low = 2 * ROWS * density
        lhs_scr[low : low + comps, :] = jnp.concatenate([poles * even, poles * odd], axis=1)
        lhs_scr[low + ROWS : low + ROWS + comps, :] = jnp.concatenate([poles * odd, -(poles * even)], axis=1)
    lhs = lhs_scr[...].astype(jnp.bfloat16)
    lhs_ref[...] = lhs
    copies[2].wait()
    structure_into(base, columns, lhs, miller_ref, form_ref, table_ref, sums_ref, copies[3].wait)
    copies[4].wait()
    copies[5].wait()
    points = owner_ref.shape[1]
    chosen = lax.broadcasted_iota(jnp.int32, (atoms, points), 0) == owner_ref[...]
    for axis in range(3):
        spread = jnp.where(chosen, columns[axis], 0.0)
        places_ref[axis : axis + 1, :] = jnp.sum(spread, axis=0, keepdims=True) + offsets_ref[axis : axis + 1, :]
    copies[6].wait()


def second_kernel(miller_ref, form_ref, lhs_ref, frac_ref, table_ref, sums_ref):
    atoms = table_ref.shape[0] // 2
    base = half_start(False, table_ref.shape[1])
    turned = frac_ref[...].T
    columns = [turned[0:atoms, axis : axis + 1] for axis in range(3)]
    structure_into(base, columns, lhs_ref[...], miller_ref, form_ref, table_ref, sums_ref, lambda: None)


def points_kernel(flip, miller_ref, places_ref, table_ref):
    width = table_ref.shape[1]
    base = half_start(flip, width)
    turned = places_ref[...].T
    columns = [turned[:, axis : axis + 1] for axis in range(3)]
    count = turned.shape[0]
    unroll = 5

    def step(index, carry):
        for inner in range(unroll):
            tables_into(table_ref, columns, miller_ref, base, (index * unroll + inner) * 128, count)
        return carry

    lax.fori_loop(0, width // (128 * unroll), step, 0)


def moments_kernel(flip, comps, *refs):
    miller_ref, form_ref, sums_ref, atoms_ref, points_ref = refs[:5]
    if flip:
        before_ref, refs = refs[5], refs[6:]
        outs, (form_scr, cos_scr, sin_scr, turned_scr) = refs[:4], refs[4:]
    else:
        out_ref, form_scr, cos_scr, sin_scr = refs[5:]
    width = atoms_ref.shape[1]
    base = half_start(flip, width)
    rows = lax.broadcasted_iota(jnp.int32, (ROWS, 128), 0)
    even = rows == comps
    for degree in range(0, 16, 2):
        even = even | ((rows >= degree * degree) & (rows < min((degree + 1) * (degree + 1), comps)))
    ones = (lax.broadcasted_iota(jnp.int32, (ROWS - comps, 128), 0) == 0).astype(jnp.float32)
    atoms = atoms_ref.shape[0] // 2
    points = points_ref.shape[0] // 2
    contract = (((1,), (1,)), ((), ()))
    total = before_ref[...] if flip else None
    chunk = width // 3
    for slot in range(form_scr.shape[0]):
        form_scr[slot, comps:ROWS, :] = ones
    for first in range(0, width, chunk):
        for start in range(first, first + chunk, 128):
            there = pl.ds(pl.multiple_of(base + start, 128), 128)
            vectors = miller_ref[:, there].astype(jnp.float32)
            square = jnp.sum(vectors * vectors, axis=0, keepdims=True)
            kernel = jnp.exp(-damping * square) / square
            potential = kernel * sums_ref[:, start : start + 128]
            slot = (start // 128) % form_scr.shape[0]
            form_scr[slot, 0:comps, :] = form_ref[:, there].astype(jnp.float32)
            form = form_scr[slot]
            against_cos, against_sin = [], []
            for density in range(2):
                real = potential[2 * density : 2 * density + 1]
                imag = potential[2 * density + 1 : 2 * density + 2]
                against_cos.append(form * jnp.where(even, real, imag))
                against_sin.append(form * jnp.where(even, -imag, real))
            cos_scr[:, start : start + 128] = jnp.concatenate(against_cos, axis=0).astype(jnp.bfloat16)
            sin_scr[:, start : start + 128] = jnp.concatenate(against_sin, axis=0).astype(jnp.bfloat16)
        span = slice(first, first + chunk)
        for part, weights in enumerate((cos_scr, sin_scr)):
            table = jnp.concatenate(
                [
                    atoms_ref[atoms * part : atoms * (part + 1), span],
                    points_ref[points * part : points * (part + 1), span],
                ],
                axis=0,
            )
            term = lax.dot_general(weights[:, span], table, contract, preferred_element_type=jnp.float32)
            total = term if total is None else total + term
    if not flip:
        out_ref[...] = total
        return
    pad = jnp.zeros((2 * ROWS, turned_scr.shape[0] - atoms - points), jnp.float32)
    turned_scr[...] = jnp.concatenate([total, pad], axis=1).T
    own = lax.axis_index("g")
    for turn, out_ref in enumerate(outs):
        few = atoms // 4
        many = points // 4
        out_ref[0:few] = turned_scr[pl.ds(pl.multiple_of((own ^ turn) * few, few), few)]
        out_ref[few : few + many] = turned_scr[atoms + many * turn : atoms + many * (turn + 1)]


def finish_kernel(comps, atoms, first_ref, second_ref, third_ref, fourth_ref, grid_ref, moments_ref):
    total = (first_ref[...] + second_ref[...]) + (third_ref[...] + fourth_ref[...])
    turned = total.T
    place = lax.broadcasted_iota(jnp.int32, (atoms, comps), 1)
    sign = jnp.zeros((atoms, comps), jnp.float32)
    degree = 0
    while degree * degree < comps:
        here = (place >= degree * degree) & (place < (degree + 1) * (degree + 1))
        sign = jnp.where(here, (1.0, -1.0, -1.0, 1.0)[degree % 4], sign)
        degree += 1
    for density in range(2):
        low = ROWS * density
        moments_ref[density] = total[0:atoms, low : low + comps] * sign
        grid_ref[density : density + 1, :] = turned[low + comps : low + comps + 1, atoms:]


def cost(flops):
    return pl.CostEstimate(flops=flops, bytes_accessed=1 << 20, transcendentals=0)


PARAMS = pltpu.CompilerParams(vmem_limit_bytes=24 << 20)


def shards(miller, form_factors, fractional, multipoles, point_owner, offsets):
    comps, vectors = form_factors.shape
    atoms = fractional.shape[1]
    half = vectors // 2
    own_points = offsets.shape[1]
    points = 4 * own_points
    few = atoms // 4
    shape = jax.ShapeDtypeStruct

    table_shapes = (shape((2 * atoms, half), jnp.bfloat16), shape((4, half), jnp.float32))
    structure_cost = cost(2 * half * 128 * 224 * 8)
    far_table, far_sums, places, miller, form_factors, lhs, frac = pl.pallas_call(
        first_kernel,
        in_specs=[pl.BlockSpec(memory_space=pltpu.HBM)] * 6,
        out_shape=(
            *table_shapes,
            shape((8, own_points), jnp.float32),
            shape(miller.shape, miller.dtype),
            shape(form_factors.shape, form_factors.dtype),
            shape((4 * ROWS, 2 * atoms), jnp.bfloat16),
            shape((8, 128), jnp.float32),
        ),
        scratch_shapes=[
            pltpu.VMEM((3, atoms), jnp.float32),
            pltpu.VMEM((comps, 2, atoms), jnp.bfloat16),
            pltpu.VMEM((1, own_points), jnp.int32),
            pltpu.VMEM((3, own_points), jnp.float32),
            pltpu.VMEM((4 * ROWS, 2 * atoms), jnp.float32),
            pltpu.SemaphoreType.DMA((7,)),
        ],
        compiler_params=PARAMS,
        cost_estimate=structure_cost,
        name="structure1",
    )(
        *[
            pltpu.with_memory_space_constraint(value, pltpu.HBM)
            for value in (
                miller, form_factors, fractional, jnp.transpose(multipoles, (1, 0, 2)), point_owner[None], offsets
            )
        ]
    )

    arrived = exchanged(far_sums, c=1)
    places = jnp.concatenate([places, exchanged(places, g=1)], axis=1)
    near_table, near_sums = pl.pallas_call(
        second_kernel,
        out_shape=table_shapes,
        compiler_params=PARAMS,
        cost_estimate=structure_cost,
        name="structure0",
    )(miller, form_factors, lhs, frac)
    sums = near_sums + arrived
    sums, places = lax.optimization_barrier((sums, places))

    def point_table(flip):
        return pl.pallas_call(
            functools.partial(points_kernel, flip),
            out_shape=shape((2 * points, half), jnp.bfloat16),
            compiler_params=PARAMS,
            cost_estimate=cost(2 * half * 128 * 224 * 8),
        )(miller, places)

    crossed = exchanged(sums, zh=1)
    others = exchanged(places, g=2)
    places = jnp.concatenate([places, others], axis=1)
    sums = sums + crossed
    far_points = point_table(1)
    near_points = point_table(0)
    for stage in (
[dict(y=1, x=3), dict(x=3), dict(y=1)],[dict(y=3, x=1), dict(y=3), dict(x=1)],
    ):
        parts = []
        for flips in stage:
            parts.append(exchanged(sums, **flips))
        for part in parts:
            sums = sums + part
    other_sums = exchanged(sums, c=1)

    def contract(flip, summed, atom_table, point_rows, before):
        if flip:
            out_shape = [shape((few + own_points, 2 * ROWS), jnp.float32)] * 4
            more = [pltpu.VMEM((256, 2 * ROWS), jnp.float32)]
        else:
            out_shape = shape((2 * ROWS, atoms + points), jnp.float32)
            more = []
        return pl.pallas_call(
            functools.partial(moments_kernel, flip, comps),
            out_shape=out_shape,
            scratch_shapes=[
                pltpu.VMEM((5, ROWS, 128), jnp.float32),
                pltpu.VMEM((2 * ROWS, half), jnp.bfloat16),
                pltpu.VMEM((2 * ROWS, half), jnp.bfloat16),
                *more,
            ],
            compiler_params=PARAMS,
            cost_estimate=cost(2 * half * 256 * 112 * 8),
        )(miller, form_factors, summed, atom_table, point_rows, *before)

    near = contract(0, sums, near_table, near_points, ())
    pieces = contract(1, other_sums, far_table, far_points, (near,))
    others = []
    for turn in (1, 2, 3):
        others.append(exchanged(pieces[turn], g=turn))
    pieces = [pieces[0]] + others
    grid, moments = pl.pallas_call(
        functools.partial(finish_kernel, comps, few),
        out_shape=[shape((2, own_points), jnp.float32), shape((2, few, comps), jnp.float32)],
        compiler_params=PARAMS,
        cost_estimate=cost(1 << 20),
        name="finish",
    )(*pieces)
    return grid, jnp.transpose(moments, (0, 2, 1))


def solution(mesh):
    fine = Mesh(mesh.devices.reshape([SIZES[axis] for axis in AXES]), AXES)
    block = ("zh", "y", "x", "c")
    placed = (
        P(None, "g"),
        P(None, "g"),
        P(None, block),
        P(None, None, block),
        P(AXES),
        P(None, AXES),
    )
    return jax.shard_map(
        shards,
        mesh=fine,
        in_specs=placed,
        out_specs=(P(None, AXES), P(None, None, AXES)),
        check_vma=False,
    )
```

```python
import functools
import itertools

import jax
import jax.numpy as jnp
from jax import lax
from jax.experimental import pallas as pl
from jax.experimental.pallas import tpu as pltpu
from jax.sharding import Mesh
from jax.sharding import PartitionSpec as P


damping = 1.0 / 400.0
AXES = ("zh", "y", "x", "c", "g")
SIZES = {"zh": 2, "y": 4, "x": 4, "c": 2, "g": 4}
ROWS = 56

SIN = (4.442883014678955, -7.308245658874512, 3.606353998184204, -0.8461104035377502, 0.10982204228639603)
COS = (1.4142135381698608, -6.978850841522217, 5.73945951461792, -1.8835527896881104, 0.3106778562068939)


def exchanged(value, **flips):
    axes = tuple(axis for axis in AXES if axis in flips)
    sizes = [SIZES[axis] for axis in axes]
    pairs = []
    for place in itertools.product(*[range(size) for size in sizes]):
        other = [at ^ flips[axis] for at, axis in zip(place, axes)]
        flat = lambda spot: functools.reduce(lambda done, pair: done * pair[1] + pair[0], zip(spot, sizes), 0)
        pairs.append((flat(place), flat(other)))
    return lax.ppermute(value, axes, pairs)


def turns(columns, indices):
    angle = columns[0] * indices[0] + columns[1] * indices[1] + columns[2] * indices[2]
    rest = angle - jnp.round(angle)
    square = rest * rest
    sine = SIN[4]
    cosine = COS[4]
    for power in (3, 2, 1, 0):
        sine = sine * square + SIN[power]
        cosine = cosine * square + COS[power]
    sine = sine * rest
    return 1.0 - sine * sine, sine * cosine


def half_start(flip, width):
    half = lax.axis_index("c")
    if flip:
        half = 1 - half
    return half * width


def tables_into(table_ref, columns, miller_ref, base, start, count):
    vectors = miller_ref[:, pl.ds(pl.multiple_of(base + start, 128), 128)].astype(jnp.float32)
    indices = [vectors[axis : axis + 1, :] for axis in range(3)]
    for low in range(0, count, 64):
        part = [values[low : low + 64] for values in columns]
        cosine, sine = turns(part, indices)
        spot = pl.ds(pl.multiple_of(start, 128), 128)
        table_ref[low : low + 64, spot] = cosine.astype(jnp.bfloat16)
        table_ref[count + low : count + low + 64, spot] = sine.astype(jnp.bfloat16)


def row_signs(comps, lanes):
    rows = lax.broadcasted_iota(jnp.int32, (comps, lanes), 0)
    even = jnp.zeros((comps, lanes), jnp.float32)
    odd = jnp.zeros((comps, lanes), jnp.float32)
    degree = 0
    while degree * degree < comps:
        here = (rows >= degree * degree) & (rows < (degree + 1) * (degree + 1))
        sign = (1.0, -1.0, -1.0, 1.0)[degree % 4]
        if degree % 2 == 0:
            even = jnp.where(here, sign, even)
        else:
            odd = jnp.where(here, sign, odd)
        degree += 1
    return even, odd


def structure_into(base, columns, lhs, miller_ref, form_ref, table_ref, sums_ref, form_ready):
    width = table_ref.shape[1]
    comps = form_ref.shape[0]
    for start in range(0, width, 256):
        cosines, sines = [], []
        for part in range(2):
            there = pl.ds(pl.multiple_of(base + start + 128 * part, 128), 128)
            vectors = miller_ref[:, there].astype(jnp.float32)
            cosine, sine = turns(columns, [vectors[axis : axis + 1, :] for axis in range(3)])
            cosines.append(cosine.astype(jnp.bfloat16))
            sines.append(sine.astype(jnp.bfloat16))
        table = jnp.concatenate([jnp.concatenate(cosines, axis=1), jnp.concatenate(sines, axis=1)], axis=0)
        table_ref[:, start : start + 256] = table
        along = jnp.dot(lhs, table, preferred_element_type=jnp.float32)
        if start == 0:
            form_ready()
        form = form_ref[:, pl.ds(pl.multiple_of(base + start, 128), 256)].astype(jnp.float32)
        for row in range(4):
            part = along[ROWS * row : ROWS * row + comps]
            sums_ref[row : row + 1, start : start + 256] = jnp.sum(form * part, axis=0, keepdims=True)


def first_kernel(
    miller_hbm, form_hbm, frac_hbm, poles_hbm, owner_hbm, offsets_hbm,
    table_ref, sums_ref, places_ref, miller_ref, form_ref, lhs_ref, frac_ref,
    frac_in, poles_ref, owner_ref, offsets_ref, lhs_scr, sems,
):
    width = table_ref.shape[1]
    comps = form_ref.shape[0]
    atoms = frac_in.shape[1]
    base = half_start(True, width)
    other = half_start(False, width)
    far = pl.ds(pl.multiple_of(base, 128), width)
    near = pl.ds(pl.multiple_of(other, 128), width)
    moves = [
        (frac_hbm, frac_in),
        (poles_hbm, poles_ref),
        (miller_hbm, miller_ref),
        (form_hbm.at[:, far], form_ref.at[:, far]),
        (owner_hbm, owner_ref),
        (offsets_hbm, offsets_ref),
        (form_hbm.at[:, near], form_ref.at[:, near]),
    ]
    copies = [pltpu.make_async_copy(start, end, sems.at[spot]) for spot, (start, end) in enumerate(moves)]
    for copy in copies:
        copy.start()
    frac_ref[...] = jnp.zeros_like(frac_ref)
    lhs_scr[...] = jnp.zeros_like(lhs_scr)
    places_ref[...] = jnp.zeros_like(places_ref)
    even, odd = row_signs(comps, atoms)
    copies[0].wait()
    frac_ref[0:3, 0:atoms] = frac_in[...]
    turned = frac_ref[...].T
    columns = [turned[0:atoms, axis : axis + 1] for axis in range(3)]
    copies[1].wait()
    for density in range(2):
        poles = poles_ref[:, density, :].astype(jnp.float32)
        low = 2 * ROWS * density
        lhs_scr[low : low + comps, :] = jnp.concatenate([poles * even, poles * odd], axis=1)
        lhs_scr[low + ROWS : low + ROWS + comps, :] = jnp.concatenate([poles * odd, -(poles * even)], axis=1)
    lhs = lhs_scr[...].astype(jnp.bfloat16)
    lhs_ref[...] = lhs
    copies[4].wait()
    copies[5].wait()
    points = owner_ref.shape[1]
    chosen = lax.broadcasted_iota(jnp.int32, (atoms, points), 0) == owner_ref[...]
    for axis in range(3):
        spread = jnp.where(chosen, columns[axis], 0.0)
        places_ref[axis : axis + 1, :] = jnp.sum(spread, axis=0, keepdims=True) + offsets_ref[axis : axis + 1, :]
    copies[2].wait()
    structure_into(base, columns, lhs, miller_ref, form_ref, table_ref, sums_ref, copies[3].wait)
    copies[6].wait()


def second_kernel(miller_ref, form_ref, lhs_ref, frac_ref, table_ref, sums_ref):
    atoms = table_ref.shape[0] // 2
    base = half_start(False, table_ref.shape[1])
    turned = frac_ref[...].T
    columns = [turned[0:atoms, axis : axis + 1] for axis in range(3)]
    structure_into(base, columns, lhs_ref[...], miller_ref, form_ref, table_ref, sums_ref, lambda: None)


def points_kernel(flip, miller_ref, places_ref, table_ref):
    width = table_ref.shape[1]
    base = half_start(flip, width)
    turned = places_ref[...].T
    columns = [turned[:, axis : axis + 1] for axis in range(3)]
    count = turned.shape[0]
    unroll = 5

    def step(index, carry):
        for inner in range(unroll):
            tables_into(table_ref, columns, miller_ref, base, (index * unroll + inner) * 128, count)
        return carry

    lax.fori_loop(0, width // (128 * unroll), step, 0)


def moments_kernel(flip, comps, *refs):
    miller_ref, form_ref, sums_ref, atoms_ref, points_ref = refs[:5]
    if flip:
        before_ref, refs = refs[5], refs[6:]
        outs, (form_scr, cos_scr, sin_scr, turned_scr) = refs[:4], refs[4:]
    else:
        out_ref, form_scr, cos_scr, sin_scr = refs[5:]
    width = atoms_ref.shape[1]
    base = half_start(flip, width)
    rows = lax.broadcasted_iota(jnp.int32, (ROWS, 128), 0)
    even = rows == comps
    for degree in range(0, 16, 2):
        even = even | ((rows >= degree * degree) & (rows < min((degree + 1) * (degree + 1), comps)))
    ones = (lax.broadcasted_iota(jnp.int32, (ROWS - comps, 128), 0) == 0).astype(jnp.float32)
    atoms = atoms_ref.shape[0] // 2
    points = points_ref.shape[0] // 2
    contract = (((1,), (1,)), ((), ()))
    total = before_ref[...] if flip else None
    chunk = width // 15
    for slot in range(form_scr.shape[0]):
        form_scr[slot, comps:ROWS, :] = ones
    for first in range(0, width, chunk):
        for start in range(first, first + chunk, 128):
            there = pl.ds(pl.multiple_of(base + start, 128), 128)
            vectors = miller_ref[:, there].astype(jnp.float32)
            square = jnp.sum(vectors * vectors, axis=0, keepdims=True)
            kernel = jnp.exp(-damping * square) / square
            potential = kernel * sums_ref[:, start : start + 128]
            slot = (start // 128) % form_scr.shape[0]
            form_scr[slot, 0:comps, :] = form_ref[:, there].astype(jnp.float32)
            form = form_scr[slot]
            against_cos, against_sin = [], []
            for density in range(2):
                real = potential[2 * density : 2 * density + 1]
                imag = potential[2 * density + 1 : 2 * density + 2]
                against_cos.append(form * jnp.where(even, real, imag))
                against_sin.append(form * jnp.where(even, -imag, real))
            cos_scr[:, start : start + 128] = jnp.concatenate(against_cos, axis=0).astype(jnp.bfloat16)
            sin_scr[:, start : start + 128] = jnp.concatenate(against_sin, axis=0).astype(jnp.bfloat16)
        span = slice(first, first + chunk)
        for part, weights in enumerate((cos_scr, sin_scr)):
            table = jnp.concatenate(
                [
                    atoms_ref[atoms * part : atoms * (part + 1), span],
                    points_ref[points * part : points * (part + 1), span],
                ],
                axis=0,
            )
            term = lax.dot_general(weights[:, span], table, contract, preferred_element_type=jnp.float32)
            total = term if total is None else total + term
    if not flip:
        out_ref[...] = total
        return
    pad = jnp.zeros((2 * ROWS, turned_scr.shape[0] - atoms - points), jnp.float32)
    turned_scr[...] = jnp.concatenate([total, pad], axis=1).T
    own = lax.axis_index("g")
    for turn, out_ref in enumerate(outs):
        few = atoms // 4
        many = points // 4
        out_ref[0:few] = turned_scr[pl.ds(pl.multiple_of((own ^ turn) * few, few), few)]
        out_ref[few : few + many] = turned_scr[atoms + many * turn : atoms + many * (turn + 1)]


def finish_kernel(comps, atoms, first_ref, second_ref, third_ref, fourth_ref, grid_ref, moments_ref):
    total = (first_ref[...] + second_ref[...]) + (third_ref[...] + fourth_ref[...])
    turned = total[atoms:].T
    place = lax.broadcasted_iota(jnp.int32, (atoms, comps), 1)
    sign = jnp.zeros((atoms, comps), jnp.float32)
    degree = 0
    while degree * degree < comps:
        here = (place >= degree * degree) & (place < (degree + 1) * (degree + 1))
        sign = jnp.where(here, (1.0, -1.0, -1.0, 1.0)[degree % 4], sign)
        degree += 1
    for density in range(2):
        low = ROWS * density
        moments_ref[density] = total[0:atoms, low : low + comps] * sign
        grid_ref[density : density + 1, :] = turned[low + comps : low + comps + 1, :]


def cost(flops):
    return pl.CostEstimate(flops=flops, bytes_accessed=1 << 20, transcendentals=0)


PARAMS = pltpu.CompilerParams(vmem_limit_bytes=24 << 20)


def shards(miller, form_factors, fractional, multipoles, point_owner, offsets):
    comps, vectors = form_factors.shape
    atoms = fractional.shape[1]
    half = vectors // 2
    own_points = offsets.shape[1]
    points = 4 * own_points
    few = atoms // 4
    shape = jax.ShapeDtypeStruct

    table_shapes = (shape((2 * atoms, half), jnp.bfloat16), shape((4, half), jnp.float32))
    structure_cost = cost(2 * half * 128 * 224 * 8)
    far_table, far_sums, places, miller, form_factors, lhs, frac = pl.pallas_call(
        first_kernel,
        in_specs=[pl.BlockSpec(memory_space=pltpu.HBM)] * 6,
        out_shape=(
            *table_shapes,
            shape((8, own_points), jnp.float32),
            shape(miller.shape, miller.dtype),
            shape(form_factors.shape, form_factors.dtype),
            shape((4 * ROWS, 2 * atoms), jnp.bfloat16),
            shape((8, 128), jnp.float32),
        ),
        scratch_shapes=[
            pltpu.VMEM((3, atoms), jnp.float32),
            pltpu.VMEM((comps, 2, atoms), jnp.bfloat16),
            pltpu.VMEM((1, own_points), jnp.int32),
            pltpu.VMEM((3, own_points), jnp.float32),
            pltpu.VMEM((4 * ROWS, 2 * atoms), jnp.float32),
            pltpu.SemaphoreType.DMA((7,)),
        ],
        compiler_params=PARAMS,
        cost_estimate=structure_cost,
        name="structure1",
    )(
        *[
            pltpu.with_memory_space_constraint(value, pltpu.HBM)
            for value in (
                miller, form_factors, fractional, jnp.transpose(multipoles, (1, 0, 2)), point_owner[None], offsets
            )
        ]
    )

    arrived = exchanged(far_sums, c=1)
    others = exchanged(places, g=1)
    places = jnp.concatenate([places, others], axis=1)
    near_table, near_sums = pl.pallas_call(
        second_kernel,
        out_shape=table_shapes,
        compiler_params=PARAMS,
        cost_estimate=structure_cost,
        name="structure0",
    )(miller, form_factors, lhs, frac)
    sums = near_sums + arrived
    sums, places = lax.optimization_barrier((sums, places))

    def point_table(flip):
        return pl.pallas_call(
            functools.partial(points_kernel, flip),
            out_shape=shape((2 * points, half), jnp.bfloat16),
            compiler_params=PARAMS,
            cost_estimate=cost(2 * half * 128 * 224 * 8),
        )(miller, places)

    crossed = exchanged(sums, zh=1)
    others = exchanged(places, g=2)
    places = jnp.concatenate([places, others], axis=1)
    sums = sums + crossed
    far_points = point_table(1)
    near_points = point_table(0)
    stages = (
        (dict(y=1, x=3), dict(x=3), dict(y=1)),
        (dict(y=3, x=1), dict(y=3), dict(x=1)),
    )
    for stage in stages:
        parts = []
        for flips in stage:
            parts.append(exchanged(sums, **flips))
        for part in parts:
            sums = sums + part
    other_sums = exchanged(sums, c=1)

    def contract(flip, summed, atom_table, point_rows, before):
        if flip:
            out_shape = [shape((few + own_points, 2 * ROWS), jnp.float32)] * 4
            more = [pltpu.VMEM((256, 2 * ROWS), jnp.float32)]
        else:
            out_shape = shape((2 * ROWS, atoms + points), jnp.float32)
            more = []
        return pl.pallas_call(
            functools.partial(moments_kernel, flip, comps),
            out_shape=out_shape,
            scratch_shapes=[
                pltpu.VMEM((5, ROWS, 128), jnp.float32),
                pltpu.VMEM((2 * ROWS, half), jnp.bfloat16),
                pltpu.VMEM((2 * ROWS, half), jnp.bfloat16),
                *more,
            ],
            compiler_params=PARAMS,
            cost_estimate=cost(2 * half * 256 * 112 * 8),
        )(miller, form_factors, summed, atom_table, point_rows, *before)

    near = contract(0, sums, near_table, near_points, ())
    pieces = contract(1, other_sums, far_table, far_points, (near,))
    others = []
    for turn in (1, 2, 3):
        others.append(exchanged(pieces[turn], g=turn))
    pieces = [pieces[0]] + others
    grid, moments = pl.pallas_call(
        functools.partial(finish_kernel, comps, few),
        out_shape=[shape((2, own_points), jnp.float32), shape((2, few, comps), jnp.float32)],
        compiler_params=PARAMS,
        cost_estimate=cost(1 << 20),
        name="finish",
    )(*pieces)
    return grid, jnp.transpose(moments, (0, 2, 1))


def solution(mesh):
    fine = Mesh(mesh.devices.reshape([SIZES[axis] for axis in AXES]), AXES)
    block = ("zh", "y", "x", "c")
    placed = (
        P(None, "g"),
        P(None, "g"),
        P(None, block),
        P(None, None, block),
        P(AXES),
        P(None, AXES),
    )
    return jax.shard_map(
        shards,
        mesh=fine,
        in_specs=placed,
        out_specs=(P(None, AXES), P(None, None, AXES)),
        check_vma=False,
    )
```
